32 devices in a mesh: fsdp: 8 (over y, x, core), tensor: 4 (over z).
Axes of the slice: x: 2, y: 2, z: 4, core: 2. Of those that a mesh axis runs over, the one named last changes fastest.
Arguments:
- new_hidden: bfloat16 [128, 2, 8192], P('fsdp'), may hold values from -6 to 6
- new_queries: bfloat16 [128, 2, 8192], P('fsdp', None, 'tensor'), may hold values from -540 to 540
- paged_cache: bfloat16 [256, 64, 2048], P('fsdp', None, 'tensor'), may hold values from -6 to 6
- block_table: int32 [128, 8], P('fsdp'), may hold values from 0 to 31
- lengths: int32 [128], P('fsdp'), may hold values from 1 to 512
- destination: int32 [128], P('fsdp'), may hold values from -1 to 7, as said below
- train_hidden: bfloat16 [512, 8192], P('fsdp'), may hold values from -6 to 6
- train_queries: bfloat16 [512, 8192], P('fsdp', 'tensor'), may hold values from -540 to 540
- documents: int32 [8, 64], P('fsdp'), may hold values from 0 to 3, never falling along the last dimension, each value on 1 to 32 neighbouring positions
- project_weight: bfloat16 [8192, 2048], P('fsdp', 'tensor'), may hold values from -0.0625 to 0.0625
- project_bias: float32 [2048], P('tensor'), may hold values from -3 to 3
Outputs:
- decoded: bfloat16 [128, 2, 8192], P('fsdp', None, 'tensor')
- train_attention: bfloat16 [512, 8192], P('fsdp', 'tensor')
- handover: bfloat16 [64, 2, 2048], P('fsdp', None, 'tensor')
The draws below stay inside these ranges and needn't reach their ends.
Inputs may be any that keep to these rules, and one draw needn't show every extreme that they name: `destination`: the rows of one fsdp index name each training shard at most once.
All inputs are finite; a program needn't handle non-finite values.
Results may differ from the reference program's by a relative error of at most 0.0095.
Values may be sent and summed in bfloat16 or wider, within the bound.
No kernel may reach another device: no remote copies, remote signals or barrier semaphores. Data moves between devices by JAX's collectives and lax.ppermute only.
A program may use at most 64 MiB of HBM per device.

```python
import math
import jax
import jax.numpy as jnp
import numpy as np
from jax import lax

D = 8192
HEADS = 64
KV_HEADS = 8
HEAD_DIM = 128
ROWS_DEV = 16
TRAIN_DEV = 64
PAGE = 64
MAX_PAGES = 8
POOL_DEV = 32
ROWS = 128
TRAIN = 512
POOL = 256
N_FSDP = 8


def draw_destination(key, part):
    groups = ROWS // ROWS_DEV
    spread_count = max(ROWS_DEV, groups)

    def per_group(group_key):
        first_key, second_key = jax.random.split(group_key)
        order = jax.random.permutation(first_key, spread_count)[:ROWS_DEV]
        finish = jax.random.randint(second_key, (ROWS_DEV,), 0, 4)
        return jnp.where((order < groups) & (finish > 0), order, -1).astype(jnp.int32)
    return jax.vmap(per_group)(jax.random.split(key, groups)).reshape(ROWS)


def draw_new_queries(key, part):
    values = jnp.clip(jax.random.normal(key, (ROWS, 2, HEADS * HEAD_DIM), jnp.float32), -6.0, 6.0)
    return values.astype(jnp.bfloat16)


def draw_train_queries(key, part):
    values = jnp.clip(jax.random.normal(key, (TRAIN, HEADS * HEAD_DIM), jnp.float32), -6.0, 6.0)
    return values.astype(jnp.bfloat16)


def set_ends(array, own_key, low, high):
    longest = array.shape.index(max(array.shape))
    spots = []
    for shift in (0, 1):
        where = [jax.random.randint(jax.random.fold_in(own_key, axis), (), 0, length) for axis, length in enumerate(array.shape)]
        where[longest] = (where[longest] + shift) % array.shape[longest]
        spots.append(tuple(where))
    return array.at[spots[0]].set(low).at[spots[1]].set(high)


def block_scale(stream_key, shape, cuts, smallest, top_value):
    gain = 1.0
    for dim, shards_of in cuts:
        steps = jax.random.uniform(jax.random.fold_in(jax.random.fold_in(stream_key, 6), dim), (shards_of,), jnp.float32, smallest / len(cuts), top_value / len(cuts))
        gain = gain * jnp.repeat(jnp.exp(steps), shape[dim] // shards_of).reshape((-1,) + (1,) * (len(shape) - 1 - dim))
    return gain


def split_up(count, total, limit, skew):
    loads = [(1 << 20) // math.isqrt(rank ** skew) + 1 for rank in range(2, count + 1)]
    surplus, given = total - limit - (count - 1), [1] * (count - 1)
    while surplus > 0:
        free = [i for i in range(count - 1) if given[i] < limit]
        pool, budget = sum([loads[i] for i in free]), surplus
        for i in free:
            extra = min(limit - given[i], max(1, budget * loads[i] // pool), surplus)
            given[i] = given[i] + extra
            surplus = surplus - extra
    return np.array([limit] + given)


def uneven_parts(own_key, amount, total, bound, lean):
    if amount == 2:
        one = jax.random.randint(own_key, (), max(1, total - bound), min(bound, total - 1) + 1)
        return jnp.stack([one, total - one])
    tallies = jnp.asarray(split_up(amount, total, bound, lean), jnp.int32)
    couples = (amount - 1) // 2
    giver, receiver = tallies[1:1 + 2 * couples:2], tallies[2:2 + 2 * couples:2]
    margin = jnp.minimum(giver - 1, bound - receiver)
    passed = jax.random.randint(jax.random.fold_in(own_key, 1), (couples,), 0, 1 << 20) % (margin + 1)
    tallies = tallies.at[1:1 + 2 * couples:2].set(giver - passed).at[2:2 + 2 * couples:2].set(receiver + passed)
    return tallies[jax.random.permutation(jax.random.fold_in(own_key, 2), amount)]


def noise(key, shape, scale, limit, cuts=(), held_as=jnp.bfloat16):
    values = jax.random.normal(key, shape, jnp.float32) * scale
    if len(cuts) > 0:
        values = block_scale(key, shape, cuts, -0.22, 0.18) * values
    return jnp.clip(values, min=-limit, max=limit).astype(held_as)


def setup_inputs(seed: int = 0) -> dict:
    seeds = jax.random.split(jax.random.key(seed), 12)
    new_hidden = noise(seeds[0], (ROWS, 2, D), 1.0, 6.0, ((0, 8),))
    new_queries = draw_new_queries(jax.random.fold_in(seeds[11], 71), 0)
    paged_cache = noise(seeds[2], (POOL, PAGE, 2 * KV_HEADS * HEAD_DIM), 1.0, 6.0, ((0, 8), (2, 4)))
    block_table = set_ends(jax.random.randint(seeds[3], (ROWS, MAX_PAGES), 0, POOL_DEV), jax.random.fold_in(seeds[3], 1), 0, POOL_DEV - 1).astype(jnp.int32)
    lengths = set_ends(jax.random.randint(seeds[4], (ROWS,), 1, PAGE * MAX_PAGES + 1), jax.random.fold_in(seeds[4], 1), 1, PAGE * MAX_PAGES).astype(jnp.int32)
    destination = draw_destination(jax.random.fold_in(seeds[11], 71), 0)
    train_hidden = noise(seeds[6], (TRAIN, D), 1.0, 6.0, ((0, 8),))
    train_queries = draw_train_queries(jax.random.fold_in(seeds[11], 71), 0)
    documents = jax.vmap(lambda own: jnp.searchsorted(jnp.cumsum(uneven_parts(own, 4, TRAIN_DEV, TRAIN_DEV // 2, 0)), jnp.arange(TRAIN_DEV), side="right"))(jax.random.split(seeds[8], N_FSDP)).reshape((N_FSDP, TRAIN_DEV)).astype(jnp.int32)
    project_weight = noise(seeds[9], (D, 2 * KV_HEADS * HEAD_DIM), D ** -0.5, 0.0625, ((0, 8), (1, 4)))
    project_bias = noise(seeds[10], (2 * KV_HEADS * HEAD_DIM,), 0.5, 3.0, ((0, 4),), jnp.float32)
    return dict(new_hidden=new_hidden, new_queries=new_queries, paged_cache=paged_cache, block_table=block_table, lengths=lengths, destination=destination, train_hidden=train_hidden, train_queries=train_queries, documents=documents, project_weight=project_weight, project_bias=project_bias)


masked_value = -1.0e30


def decode_group(operands):
    queries, tables, spans, fresh_rows, cache_pool = operands
    context = PAGE * MAX_PAGES
    group_size = HEADS // KV_HEADS
    scaling = HEAD_DIM ** -0.5
    cached = cache_pool[tables].reshape(ROWS_DEV, context, KV_HEADS, 2, HEAD_DIM).astype(jnp.float32)
    fresh_wide = fresh_rows.astype(jnp.float32)
    heads_q = queries.reshape(ROWS_DEV, 2, KV_HEADS, group_size, HEAD_DIM).astype(jnp.float32)
    old_scores = jnp.einsum('btkgd,bckd->btkgc', heads_q, cached[:, :, :, 0, :]) * scaling
    places = jnp.arange(context, dtype=jnp.int32)
    allowed_old = places[None, :] < spans[:, None]
    old_scores = jnp.where(allowed_old[:, None, None, None, :], old_scores, masked_value)
    new_scores = jnp.einsum('btkgd,bskd->btkgs', heads_q, fresh_wide[:, :, :, 0, :]) * scaling
    order = jnp.arange(2, dtype=jnp.int32)
    allowed_new = order[None, :] <= order[:, None]
    new_scores = jnp.where(allowed_new[None, :, None, None, :], new_scores, masked_value)
    highest = jnp.maximum(jnp.max(old_scores, -1, keepdims=True), jnp.max(new_scores, -1, keepdims=True))
    old_exp = jnp.exp(old_scores - highest)
    new_exp = jnp.exp(new_scores - highest)
    totals = jnp.sum(old_exp, -1, keepdims=True) + jnp.sum(new_exp, -1, keepdims=True)
    old_weights = lax.optimization_barrier((old_exp / totals).astype(jnp.bfloat16)).astype(jnp.float32)
    new_weights = lax.optimization_barrier((new_exp / totals).astype(jnp.bfloat16)).astype(jnp.float32)
    result = jnp.einsum('btkgc,bckd->btkgd', old_weights, cached[:, :, :, 1, :])
    result = result + jnp.einsum('btkgs,bskd->btkgd', new_weights, fresh_wide[:, :, :, 1, :])
    return result.astype(jnp.bfloat16).reshape(ROWS_DEV, 2, HEADS * HEAD_DIM)


def train_group(operands):
    queries, keyvals, doc_row = operands
    group_size = HEADS // KV_HEADS
    scaling = HEAD_DIM ** -0.5
    heads_q = queries.reshape(TRAIN_DEV, KV_HEADS, group_size, HEAD_DIM).astype(jnp.float32)
    wide_kv = keyvals.astype(jnp.float32)
    scores = jnp.einsum('tkgd,skd->kgts', heads_q, wide_kv[:, :, 0, :]) * scaling
    places = jnp.arange(TRAIN_DEV, dtype=jnp.int32)
    allowed = (places[None, :] <= places[:, None]) & (doc_row[None, :] == doc_row[:, None])
    scores = jnp.where(allowed[None, None, :, :], scores, masked_value)
    highest = jnp.max(scores, -1, keepdims=True)
    expo = jnp.exp(scores - highest)
    weights = expo / jnp.sum(expo, -1, keepdims=True)
    weights = lax.optimization_barrier(weights.astype(jnp.bfloat16)).astype(jnp.float32)
    result = jnp.einsum('kgts,skd->tkgd', weights, wide_kv[:, :, 1, :])
    return result.astype(jnp.bfloat16).reshape(TRAIN_DEV, HEADS * HEAD_DIM)


def reference(new_hidden, new_queries, paged_cache, block_table, lengths, destination, train_hidden, train_queries, documents, project_weight, project_bias):
    groups = N_FSDP
    columns = 2 * KV_HEADS * HEAD_DIM
    fresh = jnp.dot(new_hidden.reshape(ROWS * 2, D), project_weight, preferred_element_type=jnp.float32) + project_bias
    fresh = fresh.astype(jnp.bfloat16).reshape(ROWS, 2, KV_HEADS, 2, HEAD_DIM)
    train_kv = jnp.dot(train_hidden, project_weight, preferred_element_type=jnp.float32) + project_bias
    train_kv = train_kv.astype(jnp.bfloat16).reshape(TRAIN, KV_HEADS, 2, HEAD_DIM)
    slot_index = jnp.where(destination >= 0, destination * groups + jnp.arange(ROWS, dtype=jnp.int32) // ROWS_DEV, groups * groups).astype(jnp.int32)
    handover = jnp.zeros((groups * groups + 1, 2, columns), jnp.bfloat16).at[slot_index].set(fresh.reshape(ROWS, 2, columns))[:groups * groups]
    decoded = lax.map(decode_group, (new_queries.reshape(groups, ROWS_DEV, 2, HEADS * HEAD_DIM), block_table.reshape(groups, ROWS_DEV, MAX_PAGES), lengths.reshape(groups, ROWS_DEV), fresh.reshape(groups, ROWS_DEV, 2, KV_HEADS, 2, HEAD_DIM), paged_cache.reshape(groups, POOL_DEV, PAGE, columns)))
    decoded = decoded.reshape(ROWS, 2, HEADS * HEAD_DIM)
    train_attention = lax.map(train_group, (train_queries.reshape(groups, TRAIN_DEV, HEADS * HEAD_DIM), train_kv.reshape(groups, TRAIN_DEV, KV_HEADS, 2, HEAD_DIM), documents))
    train_attention = train_attention.reshape(TRAIN, HEADS * HEAD_DIM)
    return decoded, train_attention, handover
```

```python
import functools

import jax
import jax.numpy as jnp
from jax import lax
from jax.experimental import pallas as pl
from jax.experimental.pallas import tpu as pltpu
from jax.sharding import PartitionSpec as P


HEADS = 64
KV_HEADS = 8
HEAD_DIM = 128
GROUP = HEADS // KV_HEADS
SCALING = HEAD_DIM ** (-0.5)
MASKED = -1e30

VMEM_SPEC = pl.BlockSpec(memory_space=pltpu.VMEM)
HBM_SPEC = pl.BlockSpec(memory_space=pltpu.HBM)


def place():
    me = lax.axis_index("fsdp")
    return me % 2, me // 2


def half():
    return lax.axis_index("tensor") % 2


def column_of(row, count, repeat=1):
    shape = (count, row.shape[1])
    picked = lax.broadcasted_iota(jnp.int32, shape, 0) // repeat == lax.broadcasted_iota(
        jnp.int32, shape, 1
    )
    return jnp.sum(jnp.where(picked, row, 0), axis=1, keepdims=True)


def nt_dot(a, b):
    return lax.dot_general(a, b, (((1,), (1,)), ((), ())), preferred_element_type=jnp.float32)


def stacked(ref, head):
    lanes = [(head * GROUP + part) * HEAD_DIM for part in range(GROUP)]
    return jnp.concatenate(
        [ref[..., lane : lane + HEAD_DIM].reshape(-1, HEAD_DIM) for lane in lanes], axis=0
    )


def cached_kernel(
    page, q_hbm, cache_hbm, table_hbm, length_hbm, q_ref, acc_ref, top_ref, total_ref,
    cache_ref, table_ref, length_ref, count_ref, score_ref, sems,
):
    pairs = (
        (table_hbm, table_ref), (length_hbm, length_ref), (q_hbm, q_ref), (cache_hbm, cache_ref)
    )
    copies = [
        pltpu.make_async_copy(source, target, sems.at[index])
        for index, (source, target) in enumerate(pairs)
    ]
    for copy in copies:
        copy.start()
    for copy in copies[:2]:
        copy.wait()
    tokens, columns = cache_ref.shape
    queries = q_ref.shape[0] * 2
    local_kv = columns // (2 * HEAD_DIM)
    chunk = 256
    lane = lax.broadcasted_iota(jnp.int32, (queries, tokens), 1)
    own_page = lane // page
    offset = lane - own_page * page
    length = column_of(length_ref[...], queries, 2)
    count = jnp.zeros((queries, tokens), jnp.float32)
    for block in range(table_ref.shape[0]):
        held = (column_of(table_ref[block : block + 1, :], queries, 2) == own_page) & (
            offset < length - block * page
        )
        count = count + held.astype(jnp.float32)
    count_ref[...] = count
    for copy in copies[2:]:
        copy.wait()

    def times(start):
        return jnp.concatenate([count_ref[:, start : start + chunk]] * GROUP, axis=0)

    for head in range(local_kv):
        base = head * 2 * HEAD_DIM
        q = stacked(q_ref, head)
        top = None
        for start in range(0, tokens, chunk):
            keys = cache_ref[start : start + chunk, base : base + HEAD_DIM]
            scores = jnp.where(times(start) > 0.0, nt_dot(q, keys) * SCALING, MASKED)
            score_ref[:, start : start + chunk] = scores
            top = scores if top is None else jnp.maximum(top, scores)
        top = jnp.max(top, axis=-1, keepdims=True)
        total = jnp.zeros((GROUP * queries, chunk), jnp.float32)
        acc = jnp.zeros((GROUP * queries, HEAD_DIM), jnp.float32)
        for start in range(0, tokens, chunk):
            weights = jnp.exp(score_ref[:, start : start + chunk] - top) * times(start)
            total = total + weights
            acc = acc + jnp.dot(
                weights.astype(jnp.bfloat16),
                cache_ref[start : start + chunk, base + HEAD_DIM : base + 2 * HEAD_DIM],
                preferred_element_type=jnp.float32,
            )
        acc_ref[head] = acc
        top_ref[head] = jnp.broadcast_to(top, acc.shape)
        total_ref[head] = jnp.broadcast_to(jnp.sum(total, axis=-1, keepdims=True), acc.shape)


def slab_kernel(
    new_hbm, train_hbm, target_hbm, bias_hbm, document_hbm, *refs
):
    slabs, (bias_ref, document_ref, target_ref, sems) = refs[:8], refs[8:]
    rows = new_hbm.shape[0]
    width = slabs[0].shape[-1]
    _, chip = place()
    copies = [pltpu.make_async_copy(target_hbm, target_ref, sems.at[0])]
    for index, slab in enumerate(slabs):
        start = pl.multiple_of((chip ^ (index % 4)) * width, 128)
        if index < 4:
            source, slab = new_hbm.at[:, :, pl.ds(start, width)], slab.at[pl.ds(0, rows)]
        else:
            count = slab.shape[0]
            first = half() * count if index == 7 else 0
            source = train_hbm.at[pl.ds(first, count), pl.ds(start, width)]
        copies.append(pltpu.make_async_copy(source, slab, sems.at[1 + index]))
    copies.append(pltpu.make_async_copy(bias_hbm, bias_ref, sems.at[9]))
    copies.append(pltpu.make_async_copy(document_hbm, document_ref, sems.at[10]))
    for copy in copies:
        copy.start()
    copies[0].wait()
    target = target_ref[...].astype(jnp.float32).astype(jnp.bfloat16)
    for slab in slabs[:4]:
        slab[rows, :, :] = jnp.zeros((2, width), jnp.bfloat16)
        slab[rows, :, 0:rows] = jnp.broadcast_to(target, (2, rows))
    for copy in copies[1:]:
        copy.wait()


def halves(total):
    whole = total.astype(jnp.bfloat16)
    rest = (total - whole.astype(jnp.float32)).astype(jnp.bfloat16)
    keys = [
        rest[:, start : start + HEAD_DIM] for start in range(0, total.shape[1], 2 * HEAD_DIM)
    ]
    return jnp.concatenate([whole] + keys, axis=1)


def widened(parts):
    parts = parts.astype(jnp.float32)
    columns = parts.shape[1] * 2 // 3
    pieces = []
    for start in range(0, columns, 2 * HEAD_DIM):
        middle, rest = start + HEAD_DIM, columns + start // 2
        pieces.append(parts[:, start:middle] + parts[:, rest : rest + HEAD_DIM])
        pieces.append(parts[:, middle : middle + HEAD_DIM])
    return jnp.concatenate(pieces, axis=1)


def product(rows, weight_ref, partner_ref):
    depth = weight_ref.shape[0]
    core, _ = place()
    is_first = core == 0
    low, high = rows[:, :depth], rows[:, depth:]
    own = jnp.where(is_first, low, high)
    other = jnp.where(is_first, high, low)
    return jnp.dot(own, weight_ref[...], preferred_element_type=jnp.float32) + jnp.dot(
        other, partner_ref[...], preferred_element_type=jnp.float32
    )


def train_product_kernel(
    weight_ref, partner_ref, bias_ref, own_ref, first_ref, second_ref, near_ref, far_ref, *outs
):
    sources = (own_ref, first_ref, second_ref, near_ref, far_ref)
    count = own_ref.shape[0]
    total = product(
        jnp.concatenate([ref[...] for ref in sources], axis=0), weight_ref, partner_ref
    )
    outs[0][...] = total[:count] + bias_ref[...]
    outs[1][...] = halves(total[count : 2 * count])
    outs[2][...] = halves(total[2 * count : 3 * count])
    part = halves(total[3 * count :])
    near, far = part[: count // 2], part[count // 2 :]
    start = pl.multiple_of(half() * (count // 2), 16)
    outs[3][pl.ds(start, count // 2)] = near
    outs[3][pl.ds(pl.multiple_of(count // 2 - start, 16), count // 2)] = far


def new_product_kernel(weight_ref, partner_ref, bias_ref, *refs):
    sources, outs, kept_ref = refs[:4], refs[4:8], refs[8]
    rows = sources[0].shape[0] - 1
    count = 2 * rows
    slabs = [ref[:rows].reshape(count, ref.shape[-1]) for ref in sources]
    total = product(jnp.concatenate(slabs, axis=0), weight_ref, partner_ref)
    parts = [total[index * count : (index + 1) * count] for index in range(4)]
    parts[0] = parts[0] + bias_ref[...]
    outs[0][...] = parts[0]
    parts = [halves(part) for part in parts]
    _, chip = place()
    row = lax.broadcasted_iota(jnp.int32, (64, 1), 0)
    mask, core, seen, token = row // 16, (row // 8) % 2, (row // 2) % 4, row % 2
    shard = (2 * (chip ^ mask) + core).astype(jnp.float32)
    entry = lax.broadcasted_iota(jnp.int32, (rows, count), 0)
    lane = lax.broadcasted_iota(jnp.int32, (rows, count), 1)
    moved = None
    for index, ref in enumerate(sources):
        target = ref[rows, :, 0:rows].astype(jnp.float32)[:1]
        target = column_of(target, rows)
        target = jnp.sum(jnp.where(lane // 2 == entry, target, 0.0), axis=0, keepdims=True)
        chosen = (target == shard) & (token == lane[:1] % 2) & ((mask ^ seen) == index)
        picked = jnp.dot(
            chosen.astype(jnp.bfloat16), parts[index], preferred_element_type=jnp.float32
        )
        moved = picked if moved is None else moved + picked
    kept_ref[...] = widened(moved[:16])
    moved = moved.astype(jnp.bfloat16)
    for index in range(1, 4):
        outs[index][:count] = parts[index]
        outs[index][count:] = moved[16 * index : 16 * (index + 1)]


def pick(target_ref, fresh, shards):
    count, lanes = target_ref.shape[1], fresh.shape[0]
    row = lax.broadcasted_iota(jnp.int32, (count, lanes), 0)
    lane = lax.broadcasted_iota(jnp.int32, (count, lanes), 1)
    column = column_of(target_ref[...], count)
    target = jnp.sum(jnp.where(lane // 2 == row, column, 0), axis=0, keepdims=True)
    token = lax.broadcasted_iota(jnp.int32, (shards.shape[0], lanes), 0) % 2
    lane = lax.broadcasted_iota(jnp.int32, (shards.shape[0], lanes), 1) % 2
    chosen = (target == shards) & (token == lane)
    return jnp.dot(chosen.astype(jnp.bfloat16), fresh, preferred_element_type=jnp.float32)


def fresh_kernel(target_ref, own_ref, fresh_ref, outgoing_ref):
    fresh = own_ref[...].astype(jnp.bfloat16)
    fresh_ref[...] = fresh
    shards = lax.broadcasted_iota(jnp.int32, (2 * outgoing_ref.shape[0], 1), 0) // 2
    outgoing = pick(target_ref, fresh, shards)
    outgoing_ref[...] = outgoing.reshape(outgoing_ref.shape).astype(jnp.bfloat16)


def paired_fresh_kernel(own_ref, kept_ref, *refs):
    sources, (fresh_ref, moved_ref) = refs[:-2], refs[-2:]
    count = own_ref.shape[0]
    fresh, moved = own_ref[...], kept_ref[...]
    for ref in sources:
        arrived = widened(ref[...])
        fresh = fresh + arrived[:count]
        moved = moved + arrived[count:]
    fresh_ref[...] = fresh.astype(jnp.bfloat16)
    moved_ref[...] = moved.astype(jnp.bfloat16)


def decode_kernel(fresh_ref, q_ref, acc_ref, top_ref, total_ref, decoded_ref):
    queries = fresh_ref.shape[0]
    local_kv = fresh_ref.shape[1] // (2 * HEAD_DIM)
    row = lax.broadcasted_iota(jnp.int32, (queries, queries), 0)
    column = lax.broadcasted_iota(jnp.int32, (queries, queries), 1)
    allowed = (row // 2 == column // 2) & (column <= row)
    allowed = jnp.concatenate([allowed.astype(jnp.float32)] * GROUP, axis=0) > 0.0
    for head in range(local_kv):
        base = head * 2 * HEAD_DIM
        middle, end = base + HEAD_DIM, base + 2 * HEAD_DIM
        scores = nt_dot(stacked(q_ref, head), fresh_ref[:, base:middle]) * SCALING
        scores = jnp.where(allowed, scores, MASKED)
        old_top = top_ref[head][:, :1]
        top = jnp.maximum(old_top, jnp.max(scores, axis=-1, keepdims=True))
        shrink = jnp.exp(old_top - top)
        weights = jnp.exp(scores - top)
        total = total_ref[head][:, :1] * shrink + jnp.sum(weights, axis=-1, keepdims=True)
        result = acc_ref[head] * shrink + jnp.dot(
            weights.astype(jnp.bfloat16),
            fresh_ref[:, middle:end],
            preferred_element_type=jnp.float32,
        )
        result = result / total
        for part in range(GROUP):
            lane = (head * GROUP + part) * HEAD_DIM
            decoded_ref[:, :, lane : lane + HEAD_DIM] = (
                result[part * queries : (part + 1) * queries]
                .reshape(queries // 2, 2, HEAD_DIM)
                .astype(jnp.bfloat16)
            )


def paired_train_kernel(
    q_ref, document_ref, same_ref, other_ref, own_ref, *refs
):
    sources, (train_ref, handover_ref) = refs[:-2], refs[-2:]
    core, chip = place()
    for source, ref in ((core, same_ref), (1 - core, other_ref)):
        rows = ref[...].astype(jnp.float32)
        rows = jnp.where(core == 0, rows[:8], rows[8:])
        for mask in range(4):
            pair = rows[2 * mask : 2 * mask + 2].astype(jnp.bfloat16)
            handover_ref[2 * (chip ^ mask) + source] = pair
    total = own_ref[...]
    for ref in sources:
        total = total + widened(ref[...])
    train_attend(q_ref, document_ref, total.astype(jnp.bfloat16), train_ref)


def train_kernel(q_ref, document_ref, own_ref, train_ref):
    train_attend(q_ref, document_ref, own_ref[...].astype(jnp.bfloat16), train_ref)


def train_attend(q_ref, document_ref, keys_values, train_ref):
    tokens = q_ref.shape[0]
    local_kv = keys_values.shape[1] // (2 * HEAD_DIM)
    row = lax.broadcasted_iota(jnp.int32, (tokens, tokens), 0)
    column = lax.broadcasted_iota(jnp.int32, (tokens, tokens), 1)
    allowed = (column <= row) & (
        document_ref[...] == column_of(document_ref[...], tokens)
    )
    allowed = jnp.concatenate([allowed.astype(jnp.float32)] * GROUP, axis=0) > 0.0
    for head in range(local_kv):
        base = head * 2 * HEAD_DIM
        middle, end = base + HEAD_DIM, base + 2 * HEAD_DIM
        scores = nt_dot(stacked(q_ref, head), keys_values[:, base:middle]) * SCALING
        scores = jnp.where(allowed, scores, MASKED)
        weights = jnp.exp(scores - jnp.max(scores, axis=-1, keepdims=True))
        total = jnp.sum(weights, axis=-1, keepdims=True)
        result = jnp.dot(
            weights.astype(jnp.bfloat16),
            keys_values[:, middle:end],
            preferred_element_type=jnp.float32,
        )
        result = (result / total).astype(jnp.bfloat16)
        for part in range(GROUP):
            lane = (head * GROUP + part) * HEAD_DIM
            train_ref[:, lane : lane + HEAD_DIM] = result[part * tokens : (part + 1) * tokens]


def exchange(parts, core_groups):
    return lax.all_to_all(
        parts, "fsdp", split_axis=0, concat_axis=0, tiled=True, axis_index_groups=core_groups
    )


def call(kernel, outs, *operands, in_place=0, room=12, **options):
    single = not isinstance(outs, tuple)
    left = len(operands) - in_place
    return pl.pallas_call(
        kernel,
        out_shape=outs,
        in_specs=[HBM_SPEC] * in_place + [VMEM_SPEC] * left,
        out_specs=VMEM_SPEC if single else (VMEM_SPEC,) * len(outs),
        compiler_params=pltpu.CompilerParams(vmem_limit_bytes=room << 20),
        **options,
    )(
        *[pltpu.with_memory_space_constraint(value, pltpu.HBM) for value in operands[:in_place]],
        *operands[in_place:],
    )


def steps(
    new_hidden,
    new_queries,
    paged_cache,
    block_table,
    lengths,
    destination,
    train_hidden,
    train_queries,
    documents,
    project_weight,
    project_bias,
):
    row_count = new_hidden.shape[0]
    depth, columns = project_weight.shape
    local_kv = columns // (2 * HEAD_DIM)
    train_count = train_hidden.shape[0]
    size = lax.axis_size("fsdp")

    def swap(value):
        return lax.ppermute(value, "fsdp", [(i, i ^ 1) for i in range(size)])

    chips = size // 2
    fresh_count = row_count * 2

    def shape(dims, dtype=jnp.bfloat16):
        return jax.ShapeDtypeStruct(dims, dtype)

    pool, page, _ = paged_cache.shape
    stack = GROUP * fresh_count
    state = shape((local_kv, stack, HEAD_DIM), jnp.float32)
    tokens = pool * page
    cached_inputs = (
        new_queries,
        paged_cache.reshape(tokens, columns),
        block_table.T,
        lengths[None, :],
    )
    staged, acc, top, totals = call(
        functools.partial(cached_kernel, page),
        (shape(new_queries.shape), state, state, state),
        *cached_inputs,
        in_place=4,
        scratch_shapes=[
            pltpu.VMEM((tokens, columns), jnp.bfloat16),
            pltpu.VMEM(block_table.shape[::-1], jnp.int32),
            pltpu.VMEM((1, row_count), jnp.int32),
            pltpu.VMEM((fresh_count, tokens), jnp.float32),
            pltpu.VMEM((stack, tokens), jnp.float32),
            pltpu.SemaphoreType.DMA((4,)),
        ],
        room=24,
    )
    partner_weight = swap(project_weight)
    fresh_type = shape((fresh_count, columns))
    outgoing_type = shape((size, 2, columns))
    decode_state = (staged, acc, top, totals)
    train_inputs = (train_queries, documents)
    decoded_type, train_type = shape(new_queries.shape), shape(train_queries.shape)

    beside = lax.axis_size("tensor")
    if chips == 4 and beside % 2 == 0 and train_count % 32 == 0:
        def hop(value, mask):
            return lax.ppermute(value, "fsdp", [(i, i ^ (2 * mask)) for i in range(size)])

        wide = columns * 3 // 2

        def products(kernel, sources, rows, extra):
            outs = [shape((rows, columns), jnp.float32)] + [shape((rows + extra, wide))] * 3
            if extra:
                outs.append(shape((extra, columns), jnp.float32))
            return call(kernel, tuple(outs), project_weight, partner_weight, bias, *sources)

        others = (1, 2, 3)
        *slabs, bias, pack = call(
            slab_kernel,
            (shape((row_count + 1, 2, 2 * depth)),) * 4
            + (shape((train_count, 2 * depth)),) * 3
            + (shape((train_count // 2, 2 * depth)),)
            + (shape((1, columns), jnp.float32), shape(documents.shape, jnp.int32)),
            new_hidden,
            train_hidden,
            destination[None, :],
            project_bias[None, :],
            documents,
            in_place=5,
            scratch_shapes=[
                pltpu.VMEM((1, row_count), jnp.int32),
                pltpu.SemaphoreType.DMA((11,)),
            ],
        )
        new_slabs, train_slabs = slabs[:4], slabs[4:]
        new_rows = [hop(new_slabs[mask], mask) for mask in others]
        train_rows = [hop(train_slabs[mask], mask) for mask in others]
        own, first, second, third, kept = products(
            new_product_kernel, [new_slabs[0]] + new_rows, fresh_count, 16
        )
        back = [hop(part, mask) for mask, part in zip(others, (first, second, third))]
        fresh, same = call(
            paired_fresh_kernel, (fresh_type, shape((16, columns))), own, kept, *back
        )
        other = swap(same)
        far = lax.ppermute(train_rows[2], "tensor", [(i, i ^ 1) for i in range(beside)])
        train_own, first, second, third = products(
            train_product_kernel, [train_slabs[0]] + train_rows + [far], train_count, 0
        )
        train_back = [hop(part, mask) for mask, part in zip(others, (first, second, third))]
        decoded = call(decode_kernel, decoded_type, fresh, *decode_state)
        train_attention, handover = call(
            paired_train_kernel,
            (train_type, outgoing_type),
            train_queries,
            pack,
            same,
            other,
            train_own,
            *train_back,
        )
        return (decoded, train_attention, handover)

    def gathered(hidden):
        rows = hidden.reshape(-1, chips, 2 * depth)
        count = rows.shape[0]
        arrived = exchange(rows.transpose(1, 0, 2), groups)
        partial = jnp.dot(
            arrived.reshape(chips * count, 2 * depth),
            weight,
            preferred_element_type=jnp.float32,
        )
        partial = partial.astype(jnp.bfloat16).reshape(chips, count, columns)
        parts = exchange(partial, groups)
        return jnp.sum(parts.astype(jnp.float32), axis=0) + project_bias

    core = lax.axis_index("fsdp") % 2
    weight = jnp.where(
        core == 0,
        jnp.concatenate([project_weight, partner_weight], axis=0),
        jnp.concatenate([partner_weight, project_weight], axis=0),
    )
    groups = [[2 * c + k for c in range(chips)] for k in range(2)]
    fresh, outgoing = call(
        fresh_kernel, (fresh_type, outgoing_type), destination[None, :], gathered(new_hidden)
    )
    handover = lax.all_to_all(outgoing, "fsdp", split_axis=0, concat_axis=0, tiled=True)
    decoded = call(decode_kernel, decoded_type, fresh, *decode_state)
    train_attention = call(train_kernel, train_type, *train_inputs, gathered(train_hidden))
    return (decoded, train_attention, handover)


def solution(mesh):
    return jax.shard_map(
        steps,
        mesh=mesh,
        in_specs=(
            P("fsdp", None, None),
            P("fsdp", None, "tensor"),
            P("fsdp", None, "tensor"),
            P("fsdp", None),
            P("fsdp"),
            P("fsdp"),
            P("fsdp", None),
            P("fsdp", "tensor"),
            P("fsdp", None),
            P("fsdp", "tensor"),
            P("tensor"),
        ),
        out_specs=(P("fsdp", None, "tensor"), P("fsdp", "tensor"), P("fsdp", None, "tensor")),
        check_vma=False,
    )
```

```python
import functools

import jax
import jax.numpy as jnp
from jax import lax
from jax.experimental import pallas as pl
from jax.experimental.pallas import tpu as pltpu
from jax.sharding import PartitionSpec as P


HEADS = 64
KV_HEADS = 8
HEAD_DIM = 128
GROUP = HEADS // KV_HEADS
SCALING = HEAD_DIM ** (-0.5)
MASKED = -1e30

VMEM_SPEC = pl.BlockSpec(memory_space=pltpu.VMEM)
HBM_SPEC = pl.BlockSpec(memory_space=pltpu.HBM)


def place():
    me = lax.axis_index("fsdp")
    return me % 2, me // 2


def half():
    return lax.axis_index("tensor") % 2


def column_of(row, count, repeat=1):
    shape = (count, row.shape[1])
    picked = lax.broadcasted_iota(jnp.int32, shape, 0) // repeat == lax.broadcasted_iota(
        jnp.int32, shape, 1
    )
    return jnp.sum(jnp.where(picked, row, 0), axis=1, keepdims=True)


def nt_dot(a, b):
    return lax.dot_general(a, b, (((1,), (1,)), ((), ())), preferred_element_type=jnp.float32)


def stacked(ref, head):
    lanes = [(head * GROUP + part) * HEAD_DIM for part in range(GROUP)]
    return jnp.concatenate(
        [ref[..., lane : lane + HEAD_DIM].reshape(-1, HEAD_DIM) for lane in lanes], axis=0
    )


def cached_kernel(
    page, q_hbm, cache_hbm, table_hbm, length_hbm, q_ref, acc_ref, top_ref, total_ref,
    cache_ref, table_ref, length_ref, count_ref, score_ref, sems,
):
    pairs = (
        (table_hbm, table_ref), (length_hbm, length_ref), (q_hbm, q_ref), (cache_hbm, cache_ref)
    )
    copies = [
        pltpu.make_async_copy(source, target, sems.at[index])
        for index, (source, target) in enumerate(pairs)
    ]
    for copy in copies:
        copy.start()
    for copy in copies[:2]:
        copy.wait()
    tokens, columns = cache_ref.shape
    queries = q_ref.shape[0] * 2
    local_kv = columns // (2 * HEAD_DIM)
    chunk = 256
    lane = lax.broadcasted_iota(jnp.int32, (queries, tokens), 1)
    own_page = lane // page
    offset = lane - own_page * page
    length = column_of(length_ref[...], queries, 2)
    count = jnp.zeros((queries, tokens), jnp.float32)
    for block in range(table_ref.shape[0]):
        held = (column_of(table_ref[block : block + 1, :], queries, 2) == own_page) & (
            offset < length - block * page
        )
        count = count + held.astype(jnp.float32)
    count_ref[...] = count
    for copy in copies[2:]:
        copy.wait()

    def times(start):
        return jnp.concatenate([count_ref[:, start : start + chunk]] * GROUP, axis=0)

    for head in range(local_kv):
        base = head * 2 * HEAD_DIM
        q = stacked(q_ref, head)
        top = None
        for start in range(0, tokens, chunk):
            keys = cache_ref[start : start + chunk, base : base + HEAD_DIM]
            scores = jnp.where(times(start) > 0.0, nt_dot(q, keys) * SCALING, MASKED)
            score_ref[:, start : start + chunk] = scores
            top = scores if top is None else jnp.maximum(top, scores)
        top = jnp.max(top, axis=-1, keepdims=True)
        total = jnp.zeros((GROUP * queries, chunk), jnp.float32)
        acc = jnp.zeros((GROUP * queries, HEAD_DIM), jnp.float32)
        for start in range(0, tokens, chunk):
            weights = jnp.exp(score_ref[:, start : start + chunk] - top) * times(start)
            total = total + weights
            acc = acc + jnp.dot(
                weights.astype(jnp.bfloat16),
                cache_ref[start : start + chunk, base + HEAD_DIM : base + 2 * HEAD_DIM],
                preferred_element_type=jnp.float32,
            )
        acc_ref[head] = acc
        top_ref[head] = jnp.broadcast_to(top, acc.shape)
        total_ref[head] = jnp.broadcast_to(jnp.sum(total, axis=-1, keepdims=True), acc.shape)


def slab_kernel(
    new_hbm, train_hbm, target_hbm, bias_hbm, document_hbm, *refs
):
    slabs, (bias_ref, document_ref, target_ref, sems) = refs[:8], refs[8:]
    rows = new_hbm.shape[0]
    width = slabs[0].shape[-1]
    _, chip = place()
    copies = [pltpu.make_async_copy(target_hbm, target_ref, sems.at[0])]
    for index, slab in enumerate(slabs):
        start = pl.multiple_of((chip ^ (index % 4)) * width, 128)
        if index < 4:
            source, slab = new_hbm.at[:, :, pl.ds(start, width)], slab.at[pl.ds(0, rows)]
        else:
            count = slab.shape[0]
            first = half() * count if index == 7 else 0
            source = train_hbm.at[pl.ds(first, count), pl.ds(start, width)]
        copies.append(pltpu.make_async_copy(source, slab, sems.at[1 + index]))
    copies.append(pltpu.make_async_copy(bias_hbm, bias_ref, sems.at[9]))
    copies.append(pltpu.make_async_copy(document_hbm, document_ref, sems.at[10]))
    for copy in copies:
        copy.start()
    copies[0].wait()
    target = target_ref[...].astype(jnp.float32).astype(jnp.bfloat16)
    for slab in slabs[:4]:
        slab[rows, :, :] = jnp.zeros((2, width), jnp.bfloat16)
        slab[rows, :, 0:rows] = jnp.broadcast_to(target, (2, rows))
    for copy in copies[1:]:
        copy.wait()


def halves(total):
    whole = total.astype(jnp.bfloat16)
    rest = (total - whole.astype(jnp.float32)).astype(jnp.bfloat16)
    keys = [
        rest[:, start : start + HEAD_DIM] for start in range(0, total.shape[1], 2 * HEAD_DIM)
    ]
    return jnp.concatenate([whole] + keys, axis=1)


def widened(parts):
    parts = parts.astype(jnp.float32)
    columns = parts.shape[1] * 2 // 3
    pieces = []
    for start in range(0, columns, 2 * HEAD_DIM):
        middle, rest = start + HEAD_DIM, columns + start // 2
        pieces.append(parts[:, start:middle] + parts[:, rest : rest + HEAD_DIM])
        pieces.append(parts[:, middle : middle + HEAD_DIM])
    return jnp.concatenate(pieces, axis=1)


def product(rows, weight_ref, partner_ref):
    depth = weight_ref.shape[0]
    core, _ = place()
    is_first = core == 0
    low, high = rows[:, :depth], rows[:, depth:]
    own = jnp.where(is_first, low, high)
    other = jnp.where(is_first, high, low)
    return jnp.dot(own, weight_ref[...], preferred_element_type=jnp.float32) + jnp.dot(
        other, partner_ref[...], preferred_element_type=jnp.float32
    )


def second_product_kernel(weight_ref, partner_ref, first_ref, second_ref, *outs):
    count = first_ref.shape[0]
    rows = jnp.concatenate([first_ref[...], second_ref[...]], axis=0)
    total = product(rows, weight_ref, partner_ref)
    outs[0][...] = halves(total[:count])
    outs[1][...] = halves(total[count:])


def first_product_kernel(weight_ref, partner_ref, bias_ref, *refs):
    sources, (train_ref, near_ref, far_ref), refs = refs[:4], refs[4:7], refs[7:]
    outs, train_out, kept_ref, far_out = refs[:4], refs[4], refs[5], refs[6]
    rows = sources[0].shape[0] - 1
    count, tokens = 2 * rows, train_ref.shape[0]
    slabs = [ref[:rows].reshape(count, ref.shape[-1]) for ref in sources]
    slabs = slabs + [train_ref[...], near_ref[...], far_ref[...]]
    total = product(jnp.concatenate(slabs, axis=0), weight_ref, partner_ref)
    parts = [total[index * count : (index + 1) * count] for index in range(4)]
    parts[0] = parts[0] + bias_ref[...]
    outs[0][...] = parts[0]
    parts = [halves(part) for part in parts]
    train_out[...] = total[4 * count : 4 * count + tokens] + bias_ref[...]
    part = halves(total[4 * count + tokens :])
    middle = tokens // 2
    start = half() * middle
    far_out[pl.ds(pl.multiple_of(start, 16), middle)] = part[:middle]
    far_out[pl.ds(pl.multiple_of(middle - start, 16), middle)] = part[middle:]
    _, chip = place()
    row = lax.broadcasted_iota(jnp.int32, (64, 1), 0)
    mask, core, seen, token = row // 16, (row // 8) % 2, (row // 2) % 4, row % 2
    shard = (2 * (chip ^ mask) + core).astype(jnp.float32)
    entry = lax.broadcasted_iota(jnp.int32, (rows, count), 0)
    lane = lax.broadcasted_iota(jnp.int32, (rows, count), 1)
    moved = None
    for index, ref in enumerate(sources):
        target = ref[rows, :, 0:rows].astype(jnp.float32)[:1]
        target = column_of(target, rows)
        target = jnp.sum(jnp.where(lane // 2 == entry, target, 0.0), axis=0, keepdims=True)
        chosen = (target == shard) & (token == lane[:1] % 2) & ((mask ^ seen) == index)
        picked = jnp.dot(
            chosen.astype(jnp.bfloat16), parts[index], preferred_element_type=jnp.float32
        )
        moved = picked if moved is None else moved + picked
    kept_ref[...] = widened(moved[:16])
    moved = moved.astype(jnp.bfloat16)
    for index in range(1, 4):
        outs[index][:count] = parts[index]
        outs[index][count : count + 16] = moved[16 * index : 16 * (index + 1)]


def pick(target_ref, fresh, shards):
    count, lanes = target_ref.shape[1], fresh.shape[0]
    row = lax.broadcasted_iota(jnp.int32, (count, lanes), 0)
    lane = lax.broadcasted_iota(jnp.int32, (count, lanes), 1)
    column = column_of(target_ref[...], count)
    target = jnp.sum(jnp.where(lane // 2 == row, column, 0), axis=0, keepdims=True)
    token = lax.broadcasted_iota(jnp.int32, (shards.shape[0], lanes), 0) % 2
    lane = lax.broadcasted_iota(jnp.int32, (shards.shape[0], lanes), 1) % 2
    chosen = (target == shards) & (token == lane)
    return jnp.dot(chosen.astype(jnp.bfloat16), fresh, preferred_element_type=jnp.float32)


def fresh_kernel(target_ref, own_ref, fresh_ref, outgoing_ref):
    fresh = own_ref[...].astype(jnp.bfloat16)
    fresh_ref[...] = fresh
    shards = lax.broadcasted_iota(jnp.int32, (2 * outgoing_ref.shape[0], 1), 0) // 2
    outgoing = pick(target_ref, fresh, shards)
    outgoing_ref[...] = outgoing.reshape(outgoing_ref.shape).astype(jnp.bfloat16)


def paired_fresh_kernel(own_ref, kept_ref, *refs):
    sources, (fresh_ref, moved_ref) = refs[:-2], refs[-2:]
    count = own_ref.shape[0]
    fresh, moved = own_ref[...], kept_ref[...]
    for ref in sources:
        arrived = widened(ref[...])
        fresh = fresh + arrived[:count]
        moved = moved + arrived[count:]
    fresh_ref[...] = fresh.astype(jnp.bfloat16)
    moved_ref[...] = moved.astype(jnp.bfloat16)


def decode_kernel(fresh_ref, q_ref, acc_ref, top_ref, total_ref, decoded_ref):
    queries = fresh_ref.shape[0]
    local_kv = fresh_ref.shape[1] // (2 * HEAD_DIM)
    row = lax.broadcasted_iota(jnp.int32, (queries, queries), 0)
    column = lax.broadcasted_iota(jnp.int32, (queries, queries), 1)
    allowed = (row // 2 == column // 2) & (column <= row)
    allowed = jnp.concatenate([allowed.astype(jnp.float32)] * GROUP, axis=0) > 0.0
    for head in range(local_kv):
        base = head * 2 * HEAD_DIM
        middle, end = base + HEAD_DIM, base + 2 * HEAD_DIM
        scores = nt_dot(stacked(q_ref, head), fresh_ref[:, base:middle]) * SCALING
        scores = jnp.where(allowed, scores, MASKED)
        old_top = top_ref[head][:, :1]
        top = jnp.maximum(old_top, jnp.max(scores, axis=-1, keepdims=True))
        shrink = jnp.exp(old_top - top)
        weights = jnp.exp(scores - top)
        total = total_ref[head][:, :1] * shrink + jnp.sum(weights, axis=-1, keepdims=True)
        result = acc_ref[head] * shrink + jnp.dot(
            weights.astype(jnp.bfloat16),
            fresh_ref[:, middle:end],
            preferred_element_type=jnp.float32,
        )
        result = result / total
        for part in range(GROUP):
            lane = (head * GROUP + part) * HEAD_DIM
            decoded_ref[:, :, lane : lane + HEAD_DIM] = (
                result[part * queries : (part + 1) * queries]
                .reshape(queries // 2, 2, HEAD_DIM)
                .astype(jnp.bfloat16)
            )


def paired_train_kernel(
    q_ref, document_ref, decoded_ref, same_ref, other_ref, own_ref, *refs
):
    sources, refs = refs[:3], refs[3:]
    decoded_hbm, train_hbm, handover_hbm, train_ref, handover_ref, sems = refs
    copies = [
        pltpu.make_async_copy(source, target, sems.at[index])
        for index, (source, target) in enumerate(
            ((decoded_ref, decoded_hbm), (handover_ref, handover_hbm))
        )
    ]
    copies[0].start()
    core, chip = place()
    for source, ref in ((core, same_ref), (1 - core, other_ref)):
        rows = ref[...].astype(jnp.float32)
        rows = jnp.where(core == 0, rows[:8], rows[8:])
        for mask in range(4):
            pair = rows[2 * mask : 2 * mask + 2].astype(jnp.bfloat16)
            handover_ref[2 * (chip ^ mask) + source] = pair
    copies[1].start()
    total = own_ref[...]
    for ref in sources:
        total = total + widened(ref[...])

    def finish(head):
        lanes = pl.ds(head * GROUP * HEAD_DIM, GROUP * HEAD_DIM)
        copies.append(
            pltpu.make_async_copy(
                train_ref.at[:, lanes], train_hbm.at[:, lanes], sems.at[2 + head]
            )
        )
        copies[-1].start()

    train_attend(q_ref, document_ref, total.astype(jnp.bfloat16), train_ref, finish)
    for copy in copies:
        copy.wait()


def train_kernel(q_ref, document_ref, own_ref, train_ref):
    train_attend(
        q_ref, document_ref, own_ref[...].astype(jnp.bfloat16), train_ref, lambda head: None
    )


def train_attend(q_ref, document_ref, keys_values, train_ref, finish):
    tokens = q_ref.shape[0]
    local_kv = keys_values.shape[1] // (2 * HEAD_DIM)
    row = lax.broadcasted_iota(jnp.int32, (tokens, tokens), 0)
    column = lax.broadcasted_iota(jnp.int32, (tokens, tokens), 1)
    allowed = (column <= row) & (
        document_ref[...] == column_of(document_ref[...], tokens)
    )
    allowed = jnp.concatenate([allowed.astype(jnp.float32)] * GROUP, axis=0) > 0.0
    for head in range(local_kv):
        base = head * 2 * HEAD_DIM
        middle, end = base + HEAD_DIM, base + 2 * HEAD_DIM
        scores = nt_dot(stacked(q_ref, head), keys_values[:, base:middle]) * SCALING
        scores = jnp.where(allowed, scores, MASKED)
        weights = jnp.exp(scores - jnp.max(scores, axis=-1, keepdims=True))
        total = jnp.sum(weights, axis=-1, keepdims=True)
        result = jnp.dot(
            weights.astype(jnp.bfloat16),
            keys_values[:, middle:end],
            preferred_element_type=jnp.float32,
        )
        result = (result / total).astype(jnp.bfloat16)
        for part in range(GROUP):
            lane = (head * GROUP + part) * HEAD_DIM
            train_ref[:, lane : lane + HEAD_DIM] = result[part * tokens : (part + 1) * tokens]
        finish(head)


def exchange(parts, core_groups):
    return lax.all_to_all(
        parts, "fsdp", split_axis=0, concat_axis=0, tiled=True, axis_index_groups=core_groups
    )


def call(kernel, outs, *operands, in_place=0, out_place=False, room=12, **options):
    single = not isinstance(outs, tuple)
    left = len(operands) - in_place
    out_spec = HBM_SPEC if out_place else VMEM_SPEC
    return pl.pallas_call(
        kernel,
        out_shape=outs,
        in_specs=[HBM_SPEC] * in_place + [VMEM_SPEC] * left,
        out_specs=out_spec if single else (out_spec,) * len(outs),
        compiler_params=pltpu.CompilerParams(vmem_limit_bytes=room << 20),
        **options,
    )(
        *[pltpu.with_memory_space_constraint(value, pltpu.HBM) for value in operands[:in_place]],
        *operands[in_place:],
    )


def steps(
    new_hidden,
    new_queries,
    paged_cache,
    block_table,
    lengths,
    destination,
    train_hidden,
    train_queries,
    documents,
    project_weight,
    project_bias,
):
    row_count = new_hidden.shape[0]
    depth, columns = project_weight.shape
    local_kv = columns // (2 * HEAD_DIM)
    train_count = train_hidden.shape[0]
    size = lax.axis_size("fsdp")

    def swap(value):
        return lax.ppermute(value, "fsdp", [(i, i ^ 1) for i in range(size)])

    chips = size // 2
    fresh_count = row_count * 2

    def shape(dims, dtype=jnp.bfloat16):
        return jax.ShapeDtypeStruct(dims, dtype)

    pool, page, _ = paged_cache.shape
    stack = GROUP * fresh_count
    state = shape((local_kv, stack, HEAD_DIM), jnp.float32)
    tokens = pool * page
    cached_inputs = (
        new_queries,
        paged_cache.reshape(tokens, columns),
        block_table.T,
        lengths[None, :],
    )
    staged, acc, top, totals = call(
        functools.partial(cached_kernel, page),
        (shape(new_queries.shape), state, state, state),
        *cached_inputs,
        in_place=4,
        scratch_shapes=[
            pltpu.VMEM((tokens, columns), jnp.bfloat16),
            pltpu.VMEM(block_table.shape[::-1], jnp.int32),
            pltpu.VMEM((1, row_count), jnp.int32),
            pltpu.VMEM((fresh_count, tokens), jnp.float32),
            pltpu.VMEM((stack, tokens), jnp.float32),
            pltpu.SemaphoreType.DMA((4,)),
        ],
        room=24,
    )
    partner_weight = swap(project_weight)
    fresh_type = shape((fresh_count, columns))
    outgoing_type = shape((size, 2, columns))
    decode_state = (staged, acc, top, totals)
    train_inputs = (train_queries, documents)
    decoded_type, train_type = shape(new_queries.shape), shape(train_queries.shape)

    beside = lax.axis_size("tensor")
    if chips == 4 and beside % 2 == 0 and train_count % 32 == 0:
        def hop(value, mask):
            return lax.ppermute(value, "fsdp", [(i, i ^ (2 * mask)) for i in range(size)])

        wide = columns * 3 // 2

        others = (1, 2, 3)
        *slabs, bias, pack = call(
            slab_kernel,
            (shape((row_count + 1, 2, 2 * depth)),) * 4
            + (shape((train_count, 2 * depth)),) * 3
            + (shape((train_count // 2, 2 * depth)),)
            + (shape((1, columns), jnp.float32), shape(documents.shape, jnp.int32)),
            new_hidden,
            train_hidden,
            destination[None, :],
            project_bias[None, :],
            documents,
            in_place=5,
            scratch_shapes=[
                pltpu.VMEM((1, row_count), jnp.int32),
                pltpu.SemaphoreType.DMA((11,)),
            ],
        )
        new_slabs, train_slabs = slabs[:4], slabs[4:]
        new_rows = [hop(new_slabs[mask], mask) for mask in others]
        train_rows = [hop(train_slabs[mask], mask) for mask in others]
        far = lax.ppermute(train_rows[2], "tensor", [(i, i ^ 1) for i in range(beside)])
        weights = (project_weight, partner_weight)
        own_type = shape((fresh_count, columns), jnp.float32)
        sum_type = shape((train_count, columns), jnp.float32)
        message = fresh_count + 16
        own, first, second, third, train_own, kept, far_part = call(
            first_product_kernel,
            (
                own_type,
                shape((message, wide)),
                shape((message, wide)),
                shape((message, wide)),
                sum_type,
                shape((16, columns), jnp.float32),
                shape((train_count, wide)),
            ),
            *weights,
            bias,
            new_slabs[0],
            *new_rows,
            train_slabs[0],
            train_rows[2],
            far,
        )
        back = [hop(part, mask) for mask, part in zip(others, (first, second, third))]
        first, second = call(
            second_product_kernel, (shape((train_count, wide)),) * 2, *weights, *train_rows[:2]
        )
        train_back = [hop(part, mask) for mask, part in zip(others, (first, second, far_part))]
        fresh, same = call(
            paired_fresh_kernel, (fresh_type, shape((16, columns))), own, kept, *back
        )
        other = swap(same)
        decoded = call(decode_kernel, decoded_type, fresh, *decode_state)
        return call(
            paired_train_kernel,
            (decoded_type, train_type, outgoing_type),
            train_queries,
            pack,
            decoded,
            same,
            other,
            train_own,
            *train_back,
            out_place=True,
            scratch_shapes=[
                pltpu.VMEM(train_queries.shape, jnp.bfloat16),
                pltpu.VMEM((size, 2, columns), jnp.bfloat16),
                pltpu.SemaphoreType.DMA((2 + local_kv,)),
            ],
        )

    def gathered(hidden):
        rows = hidden.reshape(-1, chips, 2 * depth)
        count = rows.shape[0]
        arrived = exchange(rows.transpose(1, 0, 2), groups)
        partial = jnp.dot(
            arrived.reshape(chips * count, 2 * depth),
            weight,
            preferred_element_type=jnp.float32,
        )
        partial = partial.astype(jnp.bfloat16).reshape(chips, count, columns)
        parts = exchange(partial, groups)
        return jnp.sum(parts.astype(jnp.float32), axis=0) + project_bias

    core = lax.axis_index("fsdp") % 2
    weight = jnp.where(
        core == 0,
        jnp.concatenate([project_weight, partner_weight], axis=0),
        jnp.concatenate([partner_weight, project_weight], axis=0),
    )
    groups = [[2 * c + k for c in range(chips)] for k in range(2)]
    fresh, outgoing = call(
        fresh_kernel, (fresh_type, outgoing_type), destination[None, :], gathered(new_hidden)
    )
    handover = lax.all_to_all(outgoing, "fsdp", split_axis=0, concat_axis=0, tiled=True)
    decoded = call(decode_kernel, decoded_type, fresh, *decode_state)
    train_attention = call(train_kernel, train_type, *train_inputs, gathered(train_hidden))
    return (decoded, train_attention, handover)


def solution(mesh):
    return jax.shard_map(
        steps,
        mesh=mesh,
        in_specs=(
            P("fsdp", None, None),
            P("fsdp", None, "tensor"),
            P("fsdp", None, "tensor"),
            P("fsdp", None),
            P("fsdp"),
            P("fsdp"),
            P("fsdp", None),
            P("fsdp", "tensor"),
            P("fsdp", None),
            P("fsdp", "tensor"),
            P("tensor"),
        ),
        out_specs=(P("fsdp", None, "tensor"), P("fsdp", "tensor"), P("fsdp", None, "tensor")),
        check_vma=False,
    )
```

```python
import functools

import jax
import jax.numpy as jnp
from jax import lax
from jax.experimental import pallas as pl
from jax.experimental.pallas import tpu as pltpu
from jax.sharding import PartitionSpec as P


HEADS = 64
KV_HEADS = 8
HEAD_DIM = 128
GROUP = HEADS // KV_HEADS
SCALING = HEAD_DIM ** (-0.5)
MASKED = -1e30

VMEM_SPEC = pl.BlockSpec(memory_space=pltpu.VMEM)
HBM_SPEC = pl.BlockSpec(memory_space=pltpu.HBM)


def place():
    me = lax.axis_index("fsdp")
    return me % 2, me // 2


def half():
    return lax.axis_index("tensor") % 2


def column_of(row, count, repeat=1):
    shape = (count, row.shape[1])
    picked = lax.broadcasted_iota(jnp.int32, shape, 0) // repeat == lax.broadcasted_iota(
        jnp.int32, shape, 1
    )
    return jnp.sum(jnp.where(picked, row, 0), axis=1, keepdims=True)


def nt_dot(a, b):
    return lax.dot_general(a, b, (((1,), (1,)), ((), ())), preferred_element_type=jnp.float32)


def stacked(ref, head):
    lanes = [(head * GROUP + part) * HEAD_DIM for part in range(GROUP)]
    return jnp.concatenate(
        [ref[..., lane : lane + HEAD_DIM].reshape(-1, HEAD_DIM) for lane in lanes], axis=0
    )


def paired_cached_kernel(
    page, q_hbm, cache_hbm, table_hbm, length_hbm, new_hbm, train_hbm, bias_hbm, target_hbm,
    document_hbm, q_ref, acc_ref, top_ref, total_ref, new_ref, train_ref, bias_ref, target_ref,
    document_ref, cache_ref, table_ref, length_ref, count_ref, score_ref, sems, own_sems,
):
    width = new_ref.shape[-1]
    pairs = (
        (slab(new_hbm, 0, width), new_ref),
        (slab(train_hbm, 0, width), train_ref),
        (bias_hbm, bias_ref),
        (target_hbm, target_ref),
        (document_hbm, document_ref),
    )
    copies = all_started(pairs, own_sems)
    cached_kernel(
        page, q_hbm, cache_hbm, table_hbm, length_hbm, q_ref, acc_ref, top_ref, total_ref,
        cache_ref, table_ref, length_ref, count_ref, score_ref, sems,
    )
    for copy in copies:
        copy.wait()


def cached_kernel(
    page, q_hbm, cache_hbm, table_hbm, length_hbm, q_ref, acc_ref, top_ref, total_ref,
    cache_ref, table_ref, length_ref, count_ref, score_ref, sems,
):
    pairs = (
        (table_hbm, table_ref), (length_hbm, length_ref), (q_hbm, q_ref), (cache_hbm, cache_ref)
    )
    copies = all_started(pairs, sems)
    for copy in copies[:2]:
        copy.wait()
    tokens, columns = cache_ref.shape
    queries = q_ref.shape[0] * 2
    local_kv = columns // (2 * HEAD_DIM)
    chunk = 256
    lane = lax.broadcasted_iota(jnp.int32, (queries, tokens), 1)
    own_page = lane // page
    offset = lane - own_page * page
    length = column_of(length_ref[...], queries, 2)
    count = jnp.zeros((queries, tokens), jnp.float32)
    for block in range(table_ref.shape[0]):
        held = (column_of(table_ref[block : block + 1, :], queries, 2) == own_page) & (
            offset < length - block * page
        )
        count = count + held.astype(jnp.float32)
    count_ref[...] = count
    for copy in copies[2:]:
        copy.wait()

    def times(start):
        return jnp.concatenate([count_ref[:, start : start + chunk]] * GROUP, axis=0)

    for head in range(local_kv):
        base = head * 2 * HEAD_DIM
        q = stacked(q_ref, head)
        top = None
        for start in range(0, tokens, chunk):
            keys = cache_ref[start : start + chunk, base : base + HEAD_DIM]
            scores = jnp.where(times(start) > 0.0, nt_dot(q, keys) * SCALING, MASKED)
            score_ref[:, start : start + chunk] = scores
            top = scores if top is None else jnp.maximum(top, scores)
        top = jnp.max(top, axis=-1, keepdims=True)
        total = jnp.zeros((GROUP * queries, chunk), jnp.float32)
        acc = jnp.zeros((GROUP * queries, HEAD_DIM), jnp.float32)
        for start in range(0, tokens, chunk):
            weights = jnp.exp(score_ref[:, start : start + chunk] - top) * times(start)
            total = total + weights
            acc = acc + jnp.dot(
                weights.astype(jnp.bfloat16),
                cache_ref[start : start + chunk, base + HEAD_DIM : base + 2 * HEAD_DIM],
                preferred_element_type=jnp.float32,
            )
        acc_ref[head] = acc
        top_ref[head] = jnp.broadcast_to(top, acc.shape)
        total_ref[head] = jnp.broadcast_to(jnp.sum(total, axis=-1, keepdims=True), acc.shape)


def slab(source, mask, width):
    _, chip = place()
    lanes = pl.ds(pl.multiple_of((chip ^ mask) * width, 128), width)
    return source.at[:, :, lanes] if len(source.shape) == 3 else source.at[:, lanes]


def all_started(pairs, sems):
    copies = [
        pltpu.make_async_copy(source, target, sems.at[index])
        for index, (source, target) in enumerate(pairs)
    ]
    for copy in copies:
        copy.start()
    return copies


def slab_kernel(new_hbm, train_hbm, target_hbm, *refs):
    new_slabs, train_slabs, (target_ref, sems) = refs[:3], refs[3:6], refs[6:]
    rows, width = new_hbm.shape[0], train_slabs[0].shape[-1]
    count = train_slabs[2].shape[0]
    pairs = [(target_hbm, target_ref)]
    for mask, ref in enumerate(new_slabs, 1):
        pairs.append((slab(new_hbm, mask, width), ref.at[pl.ds(0, rows)]))
    for mask, ref in enumerate(train_slabs, 1):
        source = train_hbm.at[pl.ds(half() * count, count)] if mask == 3 else train_hbm
        pairs.append((slab(source, mask, width), ref))
    copies = all_started(pairs, sems)
    copies[0].wait()
    target = target_ref[...].astype(jnp.float32).astype(jnp.bfloat16)
    for ref in new_slabs:
        ref[rows, :, :] = jnp.zeros((2, width), jnp.bfloat16)
        ref[rows, :, 0:rows] = jnp.broadcast_to(target, (2, rows))
    for copy in copies[1:]:
        copy.wait()


def halves(total):
    whole = total.astype(jnp.bfloat16)
    rest = (total - whole.astype(jnp.float32)).astype(jnp.bfloat16)
    keys = [
        rest[:, start : start + HEAD_DIM] for start in range(0, total.shape[1], 2 * HEAD_DIM)
    ]
    return jnp.concatenate([whole] + keys, axis=1)


def packed(parts, columns):
    count = parts.shape[0] // 2
    rests = parts[:, columns:]
    rests = jnp.concatenate([rests[:count], rests[count:]], axis=1)
    return jnp.concatenate([parts[:, :columns], rests], axis=0)


def unpacked(rows):
    count, columns = rows.shape[0] // 3, rows.shape[1]
    rests = rows[2 * count :]
    rests = jnp.concatenate([rests[:, : columns // 2], rests[:, columns // 2 :]], axis=0)
    return widened(jnp.concatenate([rows[: 2 * count], rests], axis=1))


def widened(parts):
    parts = parts.astype(jnp.float32)
    columns = parts.shape[1] * 2 // 3
    pieces = []
    for start in range(0, columns, 2 * HEAD_DIM):
        middle, rest = start + HEAD_DIM, columns + start // 2
        pieces.append(parts[:, start:middle] + parts[:, rest : rest + HEAD_DIM])
        pieces.append(parts[:, middle : middle + HEAD_DIM])
    return jnp.concatenate(pieces, axis=1)


def product(rows, weight_ref, partner_ref):
    depth = weight_ref.shape[0]
    core, _ = place()
    is_first = core == 0
    low, high = rows[:, :depth], rows[:, depth:]
    own = jnp.where(is_first, low, high)
    other = jnp.where(is_first, high, low)
    return jnp.dot(own, weight_ref[...], preferred_element_type=jnp.float32) + jnp.dot(
        other, partner_ref[...], preferred_element_type=jnp.float32
    )


def second_product_kernel(weight_ref, partner_ref, first_ref, second_ref, *outs):
    count = first_ref.shape[0]
    rows = jnp.concatenate([first_ref[...], second_ref[...]], axis=0)
    total = product(rows, weight_ref, partner_ref)
    outs[0][...] = halves(total[:count])
    outs[1][...] = halves(total[count:])


def first_product_kernel(weight_ref, partner_ref, bias_ref, target_ref, *refs):
    sources, (train_ref, near_ref, far_ref), refs = refs[:4], refs[4:7], refs[7:]
    outs, train_out, kept_ref, far_out = refs[:4], refs[4], refs[5], refs[6]
    rows = sources[0].shape[0]
    count, tokens = 2 * rows, train_ref.shape[0]
    columns = train_out.shape[1]
    slabs = [ref[:rows].reshape(count, ref.shape[-1]) for ref in sources]
    slabs = slabs + [train_ref[...], near_ref[...], far_ref[...]]
    total = product(jnp.concatenate(slabs, axis=0), weight_ref, partner_ref)
    parts = [total[index * count : (index + 1) * count] for index in range(4)]
    parts[0] = parts[0] + bias_ref[...]
    outs[0][...] = parts[0]
    parts = [halves(part) for part in parts]
    train_out[...] = total[4 * count : 4 * count + tokens] + bias_ref[...]
    part = halves(total[4 * count + tokens :])
    middle = tokens // 2
    start = half() * middle
    far_out[pl.ds(pl.multiple_of(start, 16), middle)] = part[:middle]
    far_out[pl.ds(pl.multiple_of(middle - start, 16), middle)] = part[middle:]
    _, chip = place()
    row = lax.broadcasted_iota(jnp.int32, (64, 1), 0)
    mask, core, seen, token = row // 16, (row // 8) % 2, (row // 2) % 4, row % 2
    shard = (2 * (chip ^ mask) + core).astype(jnp.float32)
    entry = lax.broadcasted_iota(jnp.int32, (rows, count), 0)
    lane = lax.broadcasted_iota(jnp.int32, (rows, count), 1)
    moved = None
    for index, ref in enumerate(sources):
        if index == 0:
            target = target_ref[...].astype(jnp.float32)
        else:
            target = ref[rows, :, 0:rows].astype(jnp.float32)[:1]
        target = column_of(target, rows)
        target = jnp.sum(jnp.where(lane // 2 == entry, target, 0.0), axis=0, keepdims=True)
        chosen = (target == shard) & (token == lane[:1] % 2) & ((mask ^ seen) == index)
        picked = jnp.dot(
            chosen.astype(jnp.bfloat16),
            parts[index][:, :columns],
            preferred_element_type=jnp.float32,
        )
        moved = picked if moved is None else moved + picked
    kept_ref[...] = moved[:16]
    moved = moved.astype(jnp.bfloat16)
    for index in range(1, 4):
        outs[index][: 3 * rows] = packed(parts[index], columns)
        outs[index][3 * rows :] = moved[16 * index : 16 * (index + 1)]


def pick(target_ref, fresh, shards):
    count, lanes = target_ref.shape[1], fresh.shape[0]
    row = lax.broadcasted_iota(jnp.int32, (count, lanes), 0)
    lane = lax.broadcasted_iota(jnp.int32, (count, lanes), 1)
    column = column_of(target_ref[...], count)
    target = jnp.sum(jnp.where(lane // 2 == row, column, 0), axis=0, keepdims=True)
    token = lax.broadcasted_iota(jnp.int32, (shards.shape[0], lanes), 0) % 2
    lane = lax.broadcasted_iota(jnp.int32, (shards.shape[0], lanes), 1) % 2
    chosen = (target == shards) & (token == lane)
    return jnp.dot(chosen.astype(jnp.bfloat16), fresh, preferred_element_type=jnp.float32)


def fresh_kernel(target_ref, own_ref, fresh_ref, outgoing_ref):
    fresh = own_ref[...].astype(jnp.bfloat16)
    fresh_ref[...] = fresh
    shards = lax.broadcasted_iota(jnp.int32, (2 * outgoing_ref.shape[0], 1), 0) // 2
    outgoing = pick(target_ref, fresh, shards)
    outgoing_ref[...] = outgoing.reshape(outgoing_ref.shape).astype(jnp.bfloat16)


def paired_fresh_kernel(own_ref, kept_ref, *refs):
    sources, (fresh_ref, moved_ref) = refs[:-2], refs[-2:]
    count = own_ref.shape[0]
    fresh, moved = own_ref[...], kept_ref[...]
    for ref in sources:
        fresh = fresh + unpacked(ref[: count * 3 // 2])
        moved = moved + ref[count * 3 // 2 :].astype(jnp.float32)
    fresh_ref[...] = fresh.astype(jnp.bfloat16)
    moved_ref[...] = moved.astype(jnp.bfloat16)


def decode_kernel(fresh_ref, q_ref, acc_ref, top_ref, total_ref, decoded_ref):
    queries = fresh_ref.shape[0]
    local_kv = fresh_ref.shape[1] // (2 * HEAD_DIM)
    row = lax.broadcasted_iota(jnp.int32, (queries, queries), 0)
    column = lax.broadcasted_iota(jnp.int32, (queries, queries), 1)
    allowed = (row // 2 == column // 2) & (column <= row)
    allowed = jnp.concatenate([allowed.astype(jnp.float32)] * GROUP, axis=0) > 0.0
    for head in range(local_kv):
        base = head * 2 * HEAD_DIM
        middle, end = base + HEAD_DIM, base + 2 * HEAD_DIM
        scores = nt_dot(stacked(q_ref, head), fresh_ref[:, base:middle]) * SCALING
        scores = jnp.where(allowed, scores, MASKED)
        old_top = top_ref[head][:, :1]
        top = jnp.maximum(old_top, jnp.max(scores, axis=-1, keepdims=True))
        shrink = jnp.exp(old_top - top)
        weights = jnp.exp(scores - top)
        total = total_ref[head][:, :1] * shrink + jnp.sum(weights, axis=-1, keepdims=True)
        result = acc_ref[head] * shrink + jnp.dot(
            weights.astype(jnp.bfloat16),
            fresh_ref[:, middle:end],
            preferred_element_type=jnp.float32,
        )
        result = result / total
        for part in range(GROUP):
            lane = (head * GROUP + part) * HEAD_DIM
            decoded_ref[:, :, lane : lane + HEAD_DIM] = (
                result[part * queries : (part + 1) * queries]
                .reshape(queries // 2, 2, HEAD_DIM)
                .astype(jnp.bfloat16)
            )


def settle_kernel(
    document_ref, decoded_ref, same_ref, other_ref, own_ref, far_ref, decoded_hbm, handover_hbm,
    sum_ref, allowed_ref, handover_ref, sems,
):
    core, chip = place()
    for source, ref in ((core, same_ref), (1 - core, other_ref)):
        rows = ref[...].astype(jnp.float32)
        rows = jnp.where(core == 0, rows[:8], rows[8:])
        for mask in range(4):
            pair = rows[2 * mask : 2 * mask + 2].astype(jnp.bfloat16)
            handover_ref[2 * (chip ^ mask) + source] = pair
    copies = all_started(((decoded_ref, decoded_hbm), (handover_ref, handover_hbm)), sems)
    sum_ref[...] = own_ref[...] + widened(far_ref[...])
    allowed_ref[...] = allowed_pairs(document_ref)
    for copy in copies:
        copy.wait()


def paired_train_kernel(
    q_ref, allowed_ref, own_ref, first_ref, second_ref, train_hbm, train_ref, sems
):
    copies = []

    def finish(head):
        lanes = pl.ds(head * GROUP * HEAD_DIM, GROUP * HEAD_DIM)
        copies.append(
            pltpu.make_async_copy(train_ref.at[:, lanes], train_hbm.at[:, lanes], sems.at[head])
        )
        copies[-1].start()

    total = own_ref[...] + widened(first_ref[...]) + widened(second_ref[...])
    train_attend(q_ref, allowed_ref[...], total.astype(jnp.bfloat16), train_ref, finish)
    for copy in copies:
        copy.wait()


def allowed_pairs(document_ref):
    tokens = document_ref.shape[1]
    row = lax.broadcasted_iota(jnp.int32, (tokens, tokens), 0)
    column = lax.broadcasted_iota(jnp.int32, (tokens, tokens), 1)
    allowed = (column <= row) & (document_ref[...] == column_of(document_ref[...], tokens))
    return allowed.astype(jnp.float32)


def train_kernel(q_ref, document_ref, own_ref, train_ref):
    train_attend(
        q_ref,
        allowed_pairs(document_ref),
        own_ref[...].astype(jnp.bfloat16),
        train_ref,
        lambda head: None,
    )


def train_attend(q_ref, allowed, keys_values, train_ref, finish):
    tokens = q_ref.shape[0]
    local_kv = keys_values.shape[1] // (2 * HEAD_DIM)
    allowed = jnp.concatenate([allowed] * GROUP, axis=0) > 0.0
    for head in range(local_kv):
        base = head * 2 * HEAD_DIM
        middle, end = base + HEAD_DIM, base + 2 * HEAD_DIM
        scores = nt_dot(stacked(q_ref, head), keys_values[:, base:middle]) * SCALING
        scores = jnp.where(allowed, scores, MASKED)
        weights = jnp.exp(scores - jnp.max(scores, axis=-1, keepdims=True))
        total = jnp.sum(weights, axis=-1, keepdims=True)
        result = jnp.dot(
            weights.astype(jnp.bfloat16),
            keys_values[:, middle:end],
            preferred_element_type=jnp.float32,
        )
        result = (result / total).astype(jnp.bfloat16)
        for part in range(GROUP):
            lane = (head * GROUP + part) * HEAD_DIM
            train_ref[:, lane : lane + HEAD_DIM] = result[part * tokens : (part + 1) * tokens]
        finish(head)


def exchange(parts, core_groups):
    return lax.all_to_all(
        parts, "fsdp", split_axis=0, concat_axis=0, tiled=True, axis_index_groups=core_groups
    )


def call(kernel, outs, *operands, in_place=0, out_place=0, room=12, **options):
    single = not isinstance(outs, tuple)
    left = len(operands) - in_place
    out_specs = (HBM_SPEC,) * out_place + (VMEM_SPEC,) * (1 if single else len(outs) - out_place)
    return pl.pallas_call(
        kernel,
        out_shape=outs,
        in_specs=[HBM_SPEC] * in_place + [VMEM_SPEC] * left,
        out_specs=out_specs[0] if single else out_specs,
        compiler_params=pltpu.CompilerParams(vmem_limit_bytes=room << 20),
        **options,
    )(
        *[pltpu.with_memory_space_constraint(value, pltpu.HBM) for value in operands[:in_place]],
        *operands[in_place:],
    )


def steps(
    new_hidden,
    new_queries,
    paged_cache,
    block_table,
    lengths,
    destination,
    train_hidden,
    train_queries,
    documents,
    project_weight,
    project_bias,
):
    row_count = new_hidden.shape[0]
    depth, columns = project_weight.shape
    local_kv = columns // (2 * HEAD_DIM)
    train_count = train_hidden.shape[0]
    size = lax.axis_size("fsdp")

    def swap(value):
        return lax.ppermute(value, "fsdp", [(i, i ^ 1) for i in range(size)])

    chips = size // 2
    fresh_count = row_count * 2

    def shape(dims, dtype=jnp.bfloat16):
        return jax.ShapeDtypeStruct(dims, dtype)

    pool, page, _ = paged_cache.shape
    stack = GROUP * fresh_count
    state = shape((local_kv, stack, HEAD_DIM), jnp.float32)
    tokens = pool * page
    cached_inputs = (
        new_queries,
        paged_cache.reshape(tokens, columns),
        block_table.T,
        lengths[None, :],
    )
    cached_scratch = [
        pltpu.VMEM((tokens, columns), jnp.bfloat16),
        pltpu.VMEM(block_table.shape[::-1], jnp.int32),
        pltpu.VMEM((1, row_count), jnp.int32),
        pltpu.VMEM((fresh_count, tokens), jnp.float32),
        pltpu.VMEM((stack, tokens), jnp.float32),
        pltpu.SemaphoreType.DMA((4,)),
    ]
    cached_types = (shape(new_queries.shape), state, state, state)
    partner_weight = swap(project_weight)
    fresh_type = shape((fresh_count, columns))
    outgoing_type = shape((size, 2, columns))
    train_inputs = (train_queries, documents)
    decoded_type, train_type = shape(new_queries.shape), shape(train_queries.shape)

    beside = lax.axis_size("tensor")
    if chips == 4 and beside % 2 == 0 and train_count % 32 == 0:
        def hop(value, mask):
            return lax.ppermute(value, "fsdp", [(i, i ^ (2 * mask)) for i in range(size)])

        wide = columns * 3 // 2

        others = (1, 2, 3)
        staged, acc, top, totals, new_own, train_mine, bias, target, pack = call(
            functools.partial(paired_cached_kernel, page),
            cached_types
            + (
                shape((row_count, 2, 2 * depth)),
                shape((train_count, 2 * depth)),
                shape((1, columns), jnp.float32),
                shape((1, row_count), jnp.int32),
                shape(documents.shape, jnp.int32),
            ),
            *cached_inputs,
            new_hidden,
            train_hidden,
            project_bias[None, :],
            destination[None, :],
            documents,
            in_place=9,
            scratch_shapes=cached_scratch + [pltpu.SemaphoreType.DMA((5,))],
            room=24,
        )
        decode_state = (staged, acc, top, totals)
        slabs = call(
            slab_kernel,
            (shape((row_count + 1, 2, 2 * depth)),) * 3
            + (shape((train_count, 2 * depth)),) * 2
            + (shape((train_count // 2, 2 * depth)),),
            new_hidden,
            train_hidden,
            destination[None, :],
            in_place=3,
            scratch_shapes=[
                pltpu.VMEM((1, row_count), jnp.int32),
                pltpu.SemaphoreType.DMA((7,)),
            ],
        )
        new_rows = [hop(rows, mask) for mask, rows in zip(others, slabs[:3])]
        train_rows = [hop(rows, mask) for mask, rows in zip(others, slabs[3:])]
        far = lax.ppermute(train_rows[2], "tensor", [(i, i ^ 1) for i in range(beside)])
        weights = (project_weight, partner_weight)
        own_type = shape((fresh_count, columns), jnp.float32)
        sum_type = shape((train_count, columns), jnp.float32)
        message = shape((row_count * 3 + 16, columns))
        own, first, second, third, train_own, kept, far_part = call(
            first_product_kernel,
            (
                own_type,
                message,
                message,
                message,
                sum_type,
                shape((16, columns), jnp.float32),
                shape((train_count, wide)),
            ),
            *weights,
            bias,
            target,
            new_own,
            *new_rows,
            train_mine,
            train_rows[2],
            far,
        )
        back = [hop(part, mask) for mask, part in zip(others, (first, second, third))]
        first, second = call(
            second_product_kernel, (shape((train_count, wide)),) * 2, *weights, *train_rows[:2]
        )
        train_back = [hop(part, mask) for mask, part in zip(others, (first, second, far_part))]
        fresh, same = call(
            paired_fresh_kernel, (fresh_type, shape((16, columns))), own, kept, *back
        )
        other = swap(same)
        decoded = call(decode_kernel, decoded_type, fresh, *decode_state)
        decoded, handover, train_own, allowed = call(
            settle_kernel,
            (
                decoded_type,
                outgoing_type,
                sum_type,
                shape((train_count, train_count), jnp.float32),
            ),
            pack,
            decoded,
            same,
            other,
            train_own,
            train_back[2],
            out_place=2,
            scratch_shapes=[
                pltpu.VMEM((size, 2, columns), jnp.bfloat16),
                pltpu.SemaphoreType.DMA((2,)),
            ],
        )
        train_attention = call(
            paired_train_kernel,
            train_type,
            train_queries,
            allowed,
            train_own,
            *train_back[:2],
            out_place=1,
            scratch_shapes=[
                pltpu.VMEM(train_queries.shape, jnp.bfloat16),
                pltpu.SemaphoreType.DMA((local_kv,)),
            ],
        )
        return (decoded, train_attention, handover)

    decode_state = call(
        functools.partial(cached_kernel, page),
        cached_types,
        *cached_inputs,
        in_place=4,
        scratch_shapes=cached_scratch,
        room=24,
    )

    def gathered(hidden):
        rows = hidden.reshape(-1, chips, 2 * depth)
        count = rows.shape[0]
        arrived = exchange(rows.transpose(1, 0, 2), groups)
        partial = jnp.dot(
            arrived.reshape(chips * count, 2 * depth),
            weight,
            preferred_element_type=jnp.float32,
        )
        partial = partial.astype(jnp.bfloat16).reshape(chips, count, columns)
        parts = exchange(partial, groups)
        return jnp.sum(parts.astype(jnp.float32), axis=0) + project_bias

    core = lax.axis_index("fsdp") % 2
    weight = jnp.where(
        core == 0,
        jnp.concatenate([project_weight, partner_weight], axis=0),
        jnp.concatenate([partner_weight, project_weight], axis=0),
    )
    groups = [[2 * c + k for c in range(chips)] for k in range(2)]
    fresh, outgoing = call(
        fresh_kernel, (fresh_type, outgoing_type), destination[None, :], gathered(new_hidden)
    )
    handover = lax.all_to_all(outgoing, "fsdp", split_axis=0, concat_axis=0, tiled=True)
    decoded = call(decode_kernel, decoded_type, fresh, *decode_state)
    train_attention = call(train_kernel, train_type, *train_inputs, gathered(train_hidden))
    return (decoded, train_attention, handover)


def solution(mesh):
    return jax.shard_map(
        steps,
        mesh=mesh,
        in_specs=(
            P("fsdp", None, None),
            P("fsdp", None, "tensor"),
            P("fsdp", None, "tensor"),
            P("fsdp", None),
            P("fsdp"),
            P("fsdp"),
            P("fsdp", None),
            P("fsdp", "tensor"),
            P("fsdp", None),
            P("fsdp", "tensor"),
            P("tensor"),
        ),
        out_specs=(P("fsdp", None, "tensor"), P("fsdp", "tensor"), P("fsdp", None, "tensor")),
        check_vma=False,
    )
```
